128 devices in a mesh: row: 8 (over z, core), col: 4 (over y), rhs: 4 (over x).
Axes of the slice: x: 4, y: 4, z: 4, core: 2. Of those that a mesh axis runs over, the one named last changes fastest.
Arguments:
- right_side: float32 [8, 64, 8192], P('row', 'rhs', 'col'), may hold values from -6 to 6
- guess: float32 [8, 64, 8192], P('row', 'rhs', 'col'), may hold values from -6 to 6
- inverse: bfloat16 [8, 8192, 8192], P('row', 'rhs', 'col'), may hold values from -0.0625 to 0.0625
- left_factor: bfloat16 [8, 8, 64, 8192], P('row', None, None, 'col'), may hold values from -0.25 to 0.25
- right_factor: bfloat16 [8, 8, 64, 8192], P('row', None, None, 'col'), may hold values from -0.0625 to 0.0625
- ranks: int32 [8, 8], replicated, may hold values from 16 to 64
Outputs:
- solution: float32 [8, 64, 8192], P('row', 'rhs', 'col')
The draws below stay inside these ranges and needn't reach their ends.
Inputs may be any that keep to these rules, and one draw needn't show every extreme that they name: ranks[i, j] is the rank of the block in block row i and block column j; diagonal entries are not read.
All inputs are finite; a program needn't handle non-finite values.
Results may differ from the reference program's by a relative error of at most 0.008.
Values may be sent and summed in bfloat16 or wider, within the bound.
No kernel may reach another device: no remote copies, remote signals or barrier semaphores. Data moves between devices by JAX's collectives and lax.ppermute only.
A program may use at most 128 MiB of HBM per device.

```python
import jax
import jax.numpy as jnp
from jax import lax

M = 8192
K = 64
R = 64
NB = 8


def place_ends(result, rng, low, high):
    longest = result.shape.index(max(result.shape))
    spots = []
    for shift in (0, 1):
        where = [jax.random.randint(jax.random.fold_in(rng, axis), (), 0, length) for axis, length in enumerate(result.shape)]
        where[longest] = (where[longest] + shift) % result.shape[longest]
        spots.append(tuple(where))
    return result.at[spots[0]].set(low).at[spots[1]].set(high)


def block_levels(key, dims, shards, smallest, top_value):
    level, own = 1.0, jax.random.fold_in(key, 6)
    for dim, blocks in shards:
        steps = jnp.exp(jax.random.uniform(jax.random.fold_in(own, dim), (blocks,), jnp.float32, smallest / len(shards), top_value / len(shards)))
        level = level * jnp.repeat(steps, dims[dim] // blocks).reshape([-1 if axis == dim else 1 for axis in range(len(dims))])
    return level


def noise(own_key, extent, spread, bound, cuts=(), kind=jnp.bfloat16):
    factor_of = block_levels(own_key, extent, cuts, -0.22, 0.18) if cuts else 1.0
    drawn = jax.random.normal(own_key, extent, jnp.float32) * spread * factor_of
    return jnp.minimum(jnp.maximum(drawn, -bound), bound).astype(kind)


def setup_inputs(seed: int = 0) -> dict:
    arg_keys = jax.random.split(jax.random.key(seed), 7)
    return {
        "right_side": noise(arg_keys[0], (NB, R, M), 1.0, 6.0, ((0, 8), (1, 4), (2, 4)), jnp.float32),
        "guess": noise(arg_keys[1], (NB, R, M), 1.0, 6.0, ((0, 8), (1, 4), (2, 4)), jnp.float32),
        "inverse": noise(arg_keys[2], (NB, M, M), M ** -0.5, 0.0625, ((0, 8), (1, 4), (2, 4))),
        "left_factor": noise(arg_keys[3], (NB, NB, K, M), (K * NB) ** -0.5, 0.25, ((0, 8), (3, 4))),
        "right_factor": noise(arg_keys[4], (NB, NB, K, M), M ** -0.5, 0.0625, ((0, 8), (3, 4))),
        "ranks": place_ends(jax.random.randint(arg_keys[5], (NB, NB), K // 4, K + 1), jax.random.fold_in(arg_keys[5], 1), K // 4, K).astype(jnp.int32),
    }


def reference(right_side, guess, inverse, left_factor, right_factor, ranks):
    keep = (jnp.arange(K, dtype=jnp.int32)[None, None, :] < ranks[:, :, None]).astype(jnp.float32)
    keep_swap = jnp.transpose(keep, (1, 0, 2))
    right_wide = right_factor.astype(jnp.float32)
    guess_low = lax.optimization_barrier(guess.astype(jnp.bfloat16)).astype(jnp.float32)
    old_coef = jnp.einsum("jrm,jikm->jirk", guess_low, right_wide, precision=lax.Precision.HIGHEST)
    old_coef = (old_coef * keep_swap[:, :, None, :]).astype(jnp.bfloat16)
    solved = []
    new_coef = []
    for t in range(NB):
        coupled = jnp.zeros((R, M), jnp.float32)
        for j in range(NB):
            if j > t:
                coupled = coupled + jnp.dot(old_coef[j, t], left_factor[t, j], preferred_element_type=jnp.float32)
            elif j < t:
                coupled = coupled + jnp.dot(new_coef[j][t], left_factor[t, j], preferred_element_type=jnp.float32)
        residue = (right_side[t] - coupled).astype(jnp.bfloat16)
        current = jnp.dot(residue, inverse[t], preferred_element_type=jnp.float32)
        solved.append(current)
        current_low = lax.optimization_barrier(current.astype(jnp.bfloat16)).astype(jnp.float32)
        coef = jnp.einsum("rm,ikm->irk", current_low, right_wide[t], precision=lax.Precision.HIGHEST)
        new_coef.append((coef * keep[:, t][:, None, :]).astype(jnp.bfloat16))
    return jnp.stack(solved)
```

```python
import numpy as np

import jax
import jax.numpy as jnp
from jax import lax
from jax.experimental import pallas as pl
from jax.experimental.pallas import tpu as pltpu
from jax.sharding import PartitionSpec as P


NB, K, R, S = 8, 64, 64, 4
PARTS = 4
BF = jnp.bfloat16
F32 = jnp.float32


def pack_table():
    table = np.zeros((NB, 2, 16), np.int32)
    for t in range(NB):
        pairs = [(j, i) for j in range(t + 1) for i in range(t + 1, NB)]
        for s, (j, i) in enumerate(pairs):
            table[t, :, s] = (j, i)
    return table


def shift(axis_size, by):
    return [(i, (i + by) % axis_size) for i in range(axis_size)]


def pick(arrays, index):
    out = arrays[-1]
    for n in range(len(arrays) - 2, -1, -1):
        out = jnp.where(index == n, arrays[n], out)
    return out


def nt_dot(a, b):
    return lax.dot_general(a, b, (((1,), (1,)), ((), ())), preferred_element_type=F32)


def xh_kernel(meta, a_ref, inv_hbm, r_ref, old_ref, x_ref, xrs_ref, pack_ref, inv_v, h_s, sems):
    n_chunks = 4
    width = inv_v.shape[2]

    def fetch(n):
        return pltpu.make_async_copy(
            inv_hbm.at[:, pl.ds(n * width, width)], inv_v.at[n], sems.at[n]
        )

    for n in range(n_chunks):
        fetch(n).start()
    t = meta[0]
    h = None
    for n in range(n_chunks):
        fetch(n).wait()
        cols = pl.ds(n * width, width)
        x = jnp.dot(a_ref[...], inv_v[n], preferred_element_type=F32)
        low = x.astype(BF)
        x_ref[:, cols] = low
        part = nt_dot(low, r_ref[:, cols])
        if n == 0:
            for m in range(4):
                h_s[m] = part[:, m * 128 : (m + 1) * 128]
        else:
            for m in range(4):
                h_s[m] += part[:, m * 128 : (m + 1) * 128]
        xrs_ref[:, cols] = low[:64].astype(F32)
    own = pl.ds(pl.multiple_of(t * K, K), K)
    xrs_ref[...] = x_ref[own, :].astype(F32)
    for m in range(4):
        fold = jnp.dot(old_ref[...], h_s[m].astype(BF), preferred_element_type=F32)
        h_s[m, own, :] = h_s[m, own, :] - fold
    for s in range(16):
        j = meta[1 + s]
        i = meta[17 + s]
        block = h_s[i // 2, pl.ds(pl.multiple_of(j * K, K), K), :]
        swapped = pltpu.roll(block, 64, 1)
        odd = (i % 2) == 1
        even_lanes = jnp.where(odd, swapped, block)
        odd_lanes = jnp.where(odd, block, swapped)
        lane = lax.broadcasted_iota(jnp.int32, (32, 128), 1)
        pack_ref[s] = jnp.where(lane < 64, even_lanes[:32], odd_lanes[32:])


def chain_kernel(meta, ranks, hg_ref, old_ref, x_ref, xrs_ref, out_ref, c_s):
    def block(t, s):
        packed = hg_ref[t, s]
        return jnp.concatenate([packed[:, :64], packed[:, 64:]], axis=0)

    coef = {}
    lane = lax.broadcasted_iota(jnp.int32, (R, K), 1)
    c_s[0] = jnp.zeros((R, NB * K), BF)
    for t in range(NB):
        count = NB - 1 - t
        if t > 0:
            incoming = [coef[j, t] for j in range(t)]
            filler = [jnp.zeros((R, K), BF)] * (NB - t)
            c_s[t] = jnp.concatenate(incoming + filler, axis=1)
        if count == 0:
            break
        y = jnp.concatenate([block(t, t * count + b) for b in range(count)], axis=1).astype(F32)
        if t > 0:
            g = jnp.concatenate(
                [
                    jnp.concatenate([block(t, a * count + b) for b in range(count)], axis=1)
                    for a in range(t)
                ],
                axis=0,
            )
            y = y - jnp.dot(jnp.concatenate(incoming, axis=1), g, preferred_element_type=F32)
        for b in range(count):
            i = t + 1 + b
            piece = y[:, b * K : (b + 1) * K]
            coef[t, i] = jnp.where(lane < ranks[i, t], piece, 0.0).astype(BF)
    mine = meta[0]
    total = c_s[mine] + old_ref[...]
    out_ref[...] = xrs_ref[...] - jnp.dot(total, x_ref[...], preferred_element_type=F32)


def body(right_side, guess, inverse, left_factor, right_factor, ranks):
    t = lax.axis_index("row")
    q = lax.axis_index("col")
    p = lax.axis_index("rhs")
    left = left_factor[0]
    right = right_factor[0].reshape(NB * K, -1)
    m = left.shape[2]

    quarter = lax.dynamic_slice(left, (0, 16 * p, 0), (NB, 16, m))
    own_block = lax.broadcasted_iota(jnp.int32, (NB, 1, 1), 0) == t
    quarter = jnp.where(own_block, right_side[0].astype(BF)[None], quarter)
    per = NB // PARTS
    received = []
    for n in range(PARTS):
        part = quarter[n * per : (n + 1) * per]
        over_col = [part] + [lax.ppermute(part, "col", shift(S, d)) for d in range(1, S)]
        over_rhs = []
        for s in range(S):
            piece = pick(over_col, (q - p - s) % S)
            over_rhs.append(piece if s == 0 else lax.ppermute(piece, "rhs", shift(S, s)))
        ordered = [pick(over_rhs, (p - x) % S) for x in range(S)]
        received.append(jnp.stack(ordered, axis=1))
    rows = jnp.concatenate(received, axis=0).reshape(NB * K, m)

    partial_value = nt_dot(guess[0].astype(BF), right)
    sends = partial_value.reshape(S, 4, NB, K).transpose(2, 0, 1, 3).reshape(NB * S, 2, 128)
    arrived = lax.all_to_all(sends, ("row", "col"), 0, 0, tiled=True)
    old = arrived.reshape(NB, S, 4, K).sum(axis=1)
    my_ranks = lax.dynamic_index_in_dim(ranks, t, 0, keepdims=False)
    keep = lax.broadcasted_iota(jnp.int32, (NB, 1, K), 2) < my_ranks[:, None, None]
    later = lax.broadcasted_iota(jnp.int32, (NB, 1, 1), 0) > t
    old = jnp.where(keep & later, old, 0.0).astype(BF).reshape(1, NB * 2, 128)
    old = lax.all_to_all(
        jnp.broadcast_to(old, (16, NB * 2, 128)), ("rhs", "col"), 0, 0, tiled=True
    )
    old = old.reshape(16, NB, 4, K).transpose(0, 2, 1, 3).reshape(R, NB * K)

    table = jnp.asarray(pack_table())
    mine = lax.dynamic_index_in_dim(table, t, 0, keepdims=False)
    meta = jnp.concatenate([t[None].astype(jnp.int32), mine.reshape(-1)])
    vmem = pl.BlockSpec(memory_space=pltpu.VMEM)
    smem = pl.BlockSpec(memory_space=pltpu.SMEM)
    x, x_own, packed = pl.pallas_call(
        xh_kernel,
        in_specs=[smem, vmem, pl.BlockSpec(memory_space=pl.ANY), vmem, vmem],
        out_specs=[vmem, vmem, vmem],
        out_shape=[
            jax.ShapeDtypeStruct((NB * K, m), BF),
            jax.ShapeDtypeStruct((R, m), F32),
            jax.ShapeDtypeStruct((16, 32, 128), F32),
        ],
        scratch_shapes=[
            pltpu.VMEM((4, m, m // 4), BF),
            pltpu.VMEM((4, NB * K, 128), F32),
            pltpu.SemaphoreType.DMA((4,)),
        ],
        compiler_params=pltpu.CompilerParams(vmem_limit_bytes=40 * 2**20),
        name="products",
    )(meta, rows, inverse[0], right, old)

    summed = lax.all_to_all(packed, ("col", "rhs"), 0, 0, tiled=True).sum(axis=0).astype(BF)
    shared = lax.all_to_all(
        jnp.broadcast_to(summed[None], (128, 32, 128)), ("row", "col", "rhs"), 0, 0, tiled=True
    ).reshape(NB, 16, 32, 128)

    partial_solution = pl.pallas_call(
        chain_kernel,
        in_specs=[smem, smem, vmem, vmem, vmem, vmem],
        out_specs=vmem,
        out_shape=jax.ShapeDtypeStruct((R, m), F32),
        scratch_shapes=[pltpu.VMEM((NB, R, NB * K), BF)],
        compiler_params=pltpu.CompilerParams(vmem_limit_bytes=24 * 2**20),
        name="sweep",
    )(meta, ranks, shared, old, x, x_own)

    result = lax.dynamic_slice(partial_solution, (16 * p, 0), (16, m))
    for s in range(1, S):
        send = lax.dynamic_slice(partial_solution, (16 * ((p + s) % S), 0), (16, m)).astype(BF)
        result = result + lax.ppermute(send, "rhs", shift(S, s)).astype(F32)
    return result[None]


def solution(mesh):
    in_specs = (
        P("row", "rhs", "col"),
        P("row", "rhs", "col"),
        P("row", "rhs", "col"),
        P("row", None, None, "col"),
        P("row", None, None, "col"),
        P(),
    )
    out_specs = P("row", "rhs", "col")
    return jax.shard_map(body, mesh=mesh, in_specs=in_specs, out_specs=out_specs, check_vma=False)
```

```python
import numpy as np

import jax
import jax.numpy as jnp
from jax import lax
from jax.experimental import pallas as pl
from jax.experimental.pallas import tpu as pltpu
from jax.sharding import PartitionSpec as P


NB, K, R, S = 8, 64, 64, 4
PARTS = 2
HALF = NB * K // PARTS
BF = jnp.bfloat16
F32 = jnp.float32


def pack_table():
    table = np.zeros((NB, 2, 16), np.int32)
    for t in range(NB):
        pairs = [(j, i) for j in range(t + 1) for i in range(t + 1, NB)]
        for s, (j, i) in enumerate(pairs):
            table[t, :, s] = (j, i)
    return table


def shift(axis_size, by):
    return [(i, (i + by) % axis_size) for i in range(axis_size)]


def pick(arrays, index):
    out = arrays[-1]
    for n in range(len(arrays) - 2, -1, -1):
        out = jnp.where(index == n, arrays[n], out)
    return out


def nt_dot(a, b):
    return lax.dot_general(a, b, (((1,), (1,)), ((), ())), preferred_element_type=F32)


def row_copies(meta, pieces, a_ref, sems):
    copies = []
    for s, piece in enumerate(pieces):
        source = (meta[33] + (S - s)) % S
        for b in range(NB // PARTS):
            rows = pl.ds(pl.multiple_of(b * K + source * 16, 16), 16)
            copies.append(pltpu.make_async_copy(piece.at[b], a_ref.at[rows], sems.at[s, b]))
    return copies


def old_send_kernel(guess_ref, r_ref, out_ref):
    product = nt_dot(guess_ref[...].astype(BF), r_ref[...])
    left = lax.broadcasted_iota(jnp.int32, (8, 128), 1) < 64
    for m in range(NB // 2):
        upper = product[:8, m * 128 : (m + 1) * 128]
        lower = product[8:, m * 128 : (m + 1) * 128]
        even = jnp.where(left, upper, pltpu.roll(lower, 64, 1))
        odd = jnp.where(left, pltpu.roll(upper, 64, 1), lower)
        for d in range(S):
            out_ref[2 * m, d] = even
            out_ref[2 * m + 1, d] = odd


def old_sum_kernel(meta, ranks, in_ref, out_ref):
    t = meta[0]
    column = lax.broadcasted_iota(jnp.int32, (8, 128), 1) % K
    for j in range(NB):
        total = (in_ref[j, 0] + in_ref[j, 1]) + (in_ref[j, 2] + in_ref[j, 3])
        rank = jnp.where(t < j, ranks[t, j], 0)
        out_ref[j] = jnp.where(column < rank, total, 0.0).astype(BF)


def unpack_old(meta, packed, old_ref):
    left = lax.broadcasted_iota(jnp.int32, (8, 128), 1) < 64
    for s, packed_ref in enumerate(packed):
        source = (meta[33] + (S - s)) % S
        rows = pl.ds(pl.multiple_of(source * 16, 16), 16)
        for m in range(NB // 2):
            even = packed_ref[2 * m].astype(F32)
            odd = packed_ref[2 * m + 1].astype(F32)
            upper = jnp.where(left, even, pltpu.roll(odd, 64, 1))
            lower = jnp.where(left, pltpu.roll(even, 64, 1), odd)
            both = jnp.concatenate([upper, lower], axis=0).astype(BF)
            old_ref[rows, m * 128 : (m + 1) * 128] = both


def fetch_operands(inv_hbm, r_hbm, inv_v, r_v, sems):
    fetch = [
        pltpu.make_async_copy(inv_hbm.at[:, pl.ds(n * 512, 512)], inv_v.at[n], sems.at[n])
        for n in range(4)
    ]
    whole = pltpu.make_async_copy(r_hbm, r_v, sems.at[4])
    fetch[0].start()
    whole.start()
    for n in range(1, 4):
        fetch[n].start()
    return fetch, whole


def products(fetch, whole, a_ref, inv_v, r_v, x_ref, h_ref, base):
    for n in range(4):
        cols = pl.ds(n * 512, 512)
        fetch[n].wait()
        x = jnp.dot(a_ref[...], inv_v[n], preferred_element_type=F32)
        low = x.astype(BF)
        x_ref[:, cols] = low
        if n == 0:
            whole.wait()
        part = nt_dot(low, r_v[:, cols])
        for m in range(4):
            piece = part[:, m * 128 : (m + 1) * 128]
            if n == 0:
                h_ref[m, base : base + HALF] = piece
            else:
                h_ref[m, base : base + HALF] += piece


def first_kernel(
    meta, p0, p1, p2, p3, inv_hbm, r_hbm, x_ref, h_ref, a_ref, inv_v, r_v, row_sems, sems
):
    rows = row_copies(meta, (p0, p1, p2, p3), a_ref, row_sems)
    for copy in rows:
        copy.start()
    fetch, whole = fetch_operands(inv_hbm, r_hbm, inv_v, r_v, sems)
    for copy in rows:
        copy.wait()
    products(fetch, whole, a_ref, inv_v, r_v, x_ref, h_ref, 0)


def second_kernel(
    meta, p0, p1, p2, p3, inv_hbm, r_hbm, o0, o1, o2, o3, h0_ref,
    x_ref, pack_ref, old_ref, h_s, a_ref, inv_v, r_v, row_sems, sems,
):
    rows = row_copies(meta, (p0, p1, p2, p3), a_ref, row_sems)
    for copy in rows:
        copy.start()
    fetch, whole = fetch_operands(inv_hbm, r_hbm, inv_v, r_v, sems)
    unpack_old(meta, (o0, o1, o2, o3), old_ref)
    for m in range(4):
        h_s[m, :HALF] = h0_ref[m]
    for copy in rows:
        copy.wait()
    products(fetch, whole, a_ref, inv_v, r_v, x_ref, h_s, HALF)
    own = pl.ds(pl.multiple_of(meta[0] * K, K), K)
    for m in range(4):
        fold = jnp.dot(old_ref[...], h_s[m].astype(BF), preferred_element_type=F32)
        h_s[m, own, :] = h_s[m, own, :] - fold
    lane = lax.broadcasted_iota(jnp.int32, (32, 128), 1)
    for s in range(16):
        j = meta[1 + s]
        i = meta[17 + s]
        block = h_s[i // 2, pl.ds(pl.multiple_of(j * K, K), K), :]
        swapped = pltpu.roll(block, 64, 1)
        odd = (i % 2) == 1
        even_lanes = jnp.where(odd, swapped, block)
        odd_lanes = jnp.where(odd, block, swapped)
        pack_ref[s] = jnp.where(lane < 64, even_lanes[:32], odd_lanes[32:]).astype(BF)


def chain_kernel(meta, ranks, hg_ref, old_ref, x0_ref, x1_ref, out_ref, c_s):
    def block(t, s):
        packed = hg_ref[t, s]
        return jnp.concatenate([packed[:, :64], packed[:, 64:]], axis=0)

    coef = {}
    lane = lax.broadcasted_iota(jnp.int32, (R, K), 1)
    c_s[0] = jnp.zeros((R, NB * K), BF)
    for t in range(NB):
        count = NB - 1 - t
        if t > 0:
            incoming = [coef[j, t] for j in range(t)]
            filler = [jnp.zeros((R, K), BF)] * (NB - t)
            c_s[t] = jnp.concatenate(incoming + filler, axis=1)
        if count == 0:
            break
        y = jnp.concatenate([block(t, t * count + b) for b in range(count)], axis=1).astype(F32)
        if t > 0:
            g = jnp.concatenate(
                [
                    jnp.concatenate([block(t, a * count + b) for b in range(count)], axis=1)
                    for a in range(t)
                ],
                axis=0,
            )
            y = y - jnp.dot(jnp.concatenate(incoming, axis=1), g, preferred_element_type=F32)
        for b in range(count):
            i = t + 1 + b
            piece = y[:, b * K : (b + 1) * K]
            coef[t, i] = jnp.where(lane < ranks[i, t], piece, 0.0).astype(BF)
    mine = meta[0]
    total = c_s[mine] + old_ref[...]
    own = pl.ds(pl.multiple_of((mine % 4) * K, K), K)
    own_rows = jnp.where(mine < 4, x0_ref[own, :], x1_ref[own, :])
    sums = jnp.dot(total[:, :HALF], x0_ref[...], preferred_element_type=F32)
    sums = sums + jnp.dot(total[:, HALF:], x1_ref[...], preferred_element_type=F32)
    out_ref[...] = own_rows.astype(F32) - sums


def program(right_side, guess, inverse, left_factor, right_factor, ranks):
    t = lax.axis_index("row")
    q = lax.axis_index("col")
    p = lax.axis_index("rhs")
    left = left_factor[0]
    right = right_factor[0].reshape(NB * K, -1)
    m = left.shape[2]

    per = NB // PARTS
    own_rows = right_side[0].astype(BF)[None]
    parts = []
    for n in range(PARTS):
        part = lax.dynamic_slice(left, (n * per, 16 * p, 0), (per, 16, m))
        own_block = lax.broadcasted_iota(jnp.int32, (per, 1, 1), 0) + n * per == t
        parts.append(jnp.where(own_block, own_rows, part))
    parts = lax.optimization_barrier(tuple(parts))
    halves = []
    for n in range(PARTS):
        part = parts[n]
        over_col = [part] + [lax.ppermute(part, "col", shift(S, d)) for d in range(1, S)]
        over_rhs = []
        for s in range(S):
            piece = pick(over_col, (q - p - s) % S)
            over_rhs.append(piece if s == 0 else lax.ppermute(piece, "rhs", shift(S, s)))
        halves.append(over_rhs)

    table = jnp.asarray(pack_table())
    mine = lax.dynamic_index_in_dim(table, t, 0, keepdims=False)
    meta = jnp.concatenate([t[None], mine.reshape(-1), p[None]]).astype(jnp.int32)
    vmem = pl.BlockSpec(memory_space=pltpu.VMEM)
    smem = pl.BlockSpec(memory_space=pltpu.SMEM)
    sends = pl.pallas_call(
        old_send_kernel,
        in_specs=[vmem, vmem],
        out_specs=vmem,
        out_shape=jax.ShapeDtypeStruct((NB, S, 8, 128), F32),
        compiler_params=pltpu.CompilerParams(vmem_limit_bytes=8 * 2**20),
        name="old_send",
    )(guess[0], right)
    arrived = lax.all_to_all(sends.reshape(NB * S, 8, 128), ("row", "col"), 0, 0, tiled=True)
    arrived = arrived.reshape(NB, S, 8, 128)
    own_old = pl.pallas_call(
        old_sum_kernel,
        in_specs=[smem, smem, vmem],
        out_specs=vmem,
        out_shape=jax.ShapeDtypeStruct((NB, 8, 128), BF),
        compiler_params=pltpu.CompilerParams(vmem_limit_bytes=8 * 2**20),
        name="old_sum",
    )(meta, ranks, arrived)
    packed_old = [own_old] + [lax.ppermute(own_old, "rhs", shift(S, s)) for s in range(1, S)]

    hbm = pl.BlockSpec(memory_space=pltpu.HBM)
    working = [
        pltpu.VMEM((HALF, m), BF),
        pltpu.VMEM((4, m, 512), BF),
        pltpu.VMEM((NB * K, m), BF),
        pltpu.SemaphoreType.DMA((S, NB // PARTS)),
        pltpu.SemaphoreType.DMA((5,)),
    ]
    x0, h0 = pl.pallas_call(
        first_kernel,
        in_specs=[smem] + [hbm] * 6,
        out_specs=[vmem] * 2,
        out_shape=[
            jax.ShapeDtypeStruct((HALF, m), BF),
            jax.ShapeDtypeStruct((4, HALF, 128), F32),
        ],
        scratch_shapes=working,
        compiler_params=pltpu.CompilerParams(vmem_limit_bytes=53 * 2**20),
        name="first",
    )(meta, *halves[0], inverse[0], right)
    x1, packed, old = pl.pallas_call(
        second_kernel,
        in_specs=[smem] + [hbm] * 6 + [vmem] * 5,
        out_specs=[vmem] * 3,
        out_shape=[
            jax.ShapeDtypeStruct((HALF, m), BF),
            jax.ShapeDtypeStruct((16, 32, 128), BF),
            jax.ShapeDtypeStruct((R, NB * K), BF),
        ],
        scratch_shapes=[pltpu.VMEM((4, NB * K, 128), F32)] + working,
        compiler_params=pltpu.CompilerParams(vmem_limit_bytes=53 * 2**20),
        name="second",
    )(meta, *halves[1], inverse[0], right, *packed_old, h0)

    summed = lax.all_to_all(packed, ("col", "rhs"), 0, 0, tiled=True)
    summed = summed.astype(F32).sum(axis=0).astype(BF)
    shared = lax.all_to_all(
        jnp.broadcast_to(summed[None], (128, 32, 128)), ("row", "col", "rhs"), 0, 0, tiled=True
    ).reshape(NB, 16, 32, 128)

    partial_solution = pl.pallas_call(
        chain_kernel,
        in_specs=[smem, smem, vmem, vmem, vmem, vmem],
        out_specs=vmem,
        out_shape=jax.ShapeDtypeStruct((R, m), F32),
        scratch_shapes=[pltpu.VMEM((NB, R, NB * K), BF)],
        compiler_params=pltpu.CompilerParams(vmem_limit_bytes=16 * 2**20),
        name="sweep",
    )(meta, ranks, shared, old, x0, x1)

    result = lax.dynamic_slice(partial_solution, (16 * p, 0), (16, m))
    for s in range(1, S):
        send = lax.dynamic_slice(partial_solution, (16 * ((p + s) % S), 0), (16, m)).astype(BF)
        result = result + lax.ppermute(send, "rhs", shift(S, s)).astype(F32)
    return result[None]


def solution(mesh):
    in_specs = (
        P("row", "rhs", "col"),
        P("row", "rhs", "col"),
        P("row", "rhs", "col"),
        P("row", None, None, "col"),
        P("row", None, None, "col"),
        P(),
    )
    out_specs = P("row", "rhs", "col")
    return jax.shard_map(program, mesh=mesh, in_specs=in_specs, out_specs=out_specs, check_vma=False)
```

```python
import numpy as np

import jax
import jax.numpy as jnp
from jax import lax
from jax.experimental import pallas as pl
from jax.experimental.pallas import tpu as pltpu
from jax.sharding import PartitionSpec as P


NB, K, R, S = 8, 64, 64, 4
PARTS = 2
HALF = NB * K // PARTS
BF = jnp.bfloat16
F32 = jnp.float32


def pack_table():
    table = np.zeros((NB, 2, 16), np.int32)
    for t in range(NB):
        pairs = [(j, i) for j in range(t + 1) for i in range(t + 1, NB)]
        for s, (j, i) in enumerate(pairs):
            table[t, :, s] = (j, i)
    return table


def shift(axis_size, by):
    return [(i, (i + by) % axis_size) for i in range(axis_size)]


def pick(arrays, index):
    out = arrays[-1]
    for n in range(len(arrays) - 2, -1, -1):
        out = jnp.where(index == n, arrays[n], out)
    return out


def nt_dot(a, b):
    return lax.dot_general(a, b, (((1,), (1,)), ((), ())), preferred_element_type=F32)


def old_send_kernel(guess_ref, r_ref, out_ref):
    product = nt_dot(guess_ref[...].astype(BF), r_ref[...])
    left = lax.broadcasted_iota(jnp.int32, (8, 128), 1) < 64
    for m in range(NB // 2):
        upper = product[:8, m * 128 : (m + 1) * 128]
        lower = product[8:, m * 128 : (m + 1) * 128]
        even = jnp.where(left, upper, pltpu.roll(lower, 64, 1))
        odd = jnp.where(left, pltpu.roll(upper, 64, 1), lower)
        for d in range(S):
            out_ref[2 * m, d] = even
            out_ref[2 * m + 1, d] = odd


def old_sum_kernel(meta, ranks, in_ref, out_ref):
    t = meta[0]
    column = lax.broadcasted_iota(jnp.int32, (8, 128), 1) % K
    for j in range(NB):
        total = (in_ref[j, 0] + in_ref[j, 1]) + (in_ref[j, 2] + in_ref[j, 3])
        rank = jnp.where(t < j, ranks[t, j], 0)
        out_ref[j] = jnp.where(column < rank, total, 0.0).astype(BF)


def unpack_old(meta, packed, old_ref):
    left = lax.broadcasted_iota(jnp.int32, (8, 128), 1) < 64
    for s, packed_ref in enumerate(packed):
        source = (meta[33] + (S - s)) % S
        rows = pl.ds(pl.multiple_of(source * 16, 16), 16)
        for m in range(NB // 2):
            even = packed_ref[2 * m].astype(F32)
            odd = packed_ref[2 * m + 1].astype(F32)
            upper = jnp.where(left, even, pltpu.roll(odd, 64, 1))
            lower = jnp.where(left, pltpu.roll(even, 64, 1), odd)
            both = jnp.concatenate([upper, lower], axis=0).astype(BF)
            old_ref[rows, m * 128 : (m + 1) * 128] = both


def first_kernel(a_ref, inv_ref, r_ref, x_ref, h_ref):
    x_ref[...] = jnp.dot(a_ref[...], inv_ref[...], preferred_element_type=F32).astype(BF)
    part = nt_dot(x_ref[...], r_ref[...])
    for m in range(4):
        h_ref[m] = part[:, m * 128 : (m + 1) * 128]


def second_kernel(
    meta, a_ref, inv_ref, r_ref, o0, o1, o2, o3, h0_ref, x_ref, pack_ref, old_ref, h_s
):
    unpack_old(meta, (o0, o1, o2, o3), old_ref)
    for m in range(4):
        h_s[m, :HALF] = h0_ref[m]
    x_ref[...] = jnp.dot(a_ref[...], inv_ref[...], preferred_element_type=F32).astype(BF)
    part = nt_dot(x_ref[...], r_ref[...])
    for m in range(4):
        h_s[m, HALF:] = part[:, m * 128 : (m + 1) * 128]
    own = pl.ds(pl.multiple_of(meta[0] * K, K), K)
    for m in range(4):
        fold = jnp.dot(old_ref[...], h_s[m].astype(BF), preferred_element_type=F32)
        h_s[m, own, :] = h_s[m, own, :] - fold
    lane = lax.broadcasted_iota(jnp.int32, (32, 128), 1)
    for s in range(16):
        j = meta[1 + s]
        i = meta[17 + s]
        block = h_s[i // 2, pl.ds(pl.multiple_of(j * K, K), K), :]
        swapped = pltpu.roll(block, 64, 1)
        odd = (i % 2) == 1
        even_lanes = jnp.where(odd, swapped, block)
        odd_lanes = jnp.where(odd, block, swapped)
        pack_ref[s] = jnp.where(lane < 64, even_lanes[:32], odd_lanes[32:]).astype(BF)


def chain_kernel(meta, ranks, hg_ref, old_ref, x0_ref, x1_ref, out_ref, c_s):
    def block(t, s):
        packed = hg_ref[t, s]
        return jnp.concatenate([packed[:, :64], packed[:, 64:]], axis=0)

    coef = {}
    lane = lax.broadcasted_iota(jnp.int32, (R, K), 1)
    c_s[0] = jnp.zeros((R, NB * K), BF)
    for t in range(NB):
        count = NB - 1 - t
        if t > 0:
            incoming = [coef[j, t] for j in range(t)]
            filler = [jnp.zeros((R, K), BF)] * (NB - t)
            c_s[t] = jnp.concatenate(incoming + filler, axis=1)
        if count == 0:
            break
        y = jnp.concatenate([block(t, t * count + b) for b in range(count)], axis=1).astype(F32)
        if t > 0:
            g = jnp.concatenate(
                [
                    jnp.concatenate([block(t, a * count + b) for b in range(count)], axis=1)
                    for a in range(t)
                ],
                axis=0,
            )
            y = y - jnp.dot(jnp.concatenate(incoming, axis=1), g, preferred_element_type=F32)
        for b in range(count):
            i = t + 1 + b
            piece = y[:, b * K : (b + 1) * K]
            coef[t, i] = jnp.where(lane < ranks[i, t], piece, 0.0).astype(BF)
    mine = meta[0]
    total = c_s[mine] + old_ref[...]
    own = pl.ds(pl.multiple_of((mine % 4) * K, K), K)
    own_rows = jnp.where(mine < 4, x0_ref[own, :], x1_ref[own, :])
    sums = jnp.dot(total[:, :HALF], x0_ref[...], preferred_element_type=F32)
    sums = sums + jnp.dot(total[:, HALF:], x1_ref[...], preferred_element_type=F32)
    out_ref[...] = own_rows.astype(F32) - sums


def program(right_side, guess, inverse, left_factor, right_factor, ranks):
    t = lax.axis_index("row")
    q = lax.axis_index("col")
    p = lax.axis_index("rhs")
    left = left_factor[0]
    right = right_factor[0].reshape(NB * K, -1)
    m = left.shape[2]

    per = NB // PARTS
    own_rows = right_side[0].astype(BF)[None]
    parts = []
    for n in range(PARTS):
        part = lax.dynamic_slice(left, (n * per, 16 * p, 0), (per, 16, m))
        own_block = lax.broadcasted_iota(jnp.int32, (per, 1, 1), 0) + n * per == t
        parts.append(jnp.where(own_block, own_rows, part))
    parts = lax.optimization_barrier(tuple(parts))
    halves = []
    for n in range(PARTS):
        part = parts[n]
        over_col = [part] + [lax.ppermute(part, "col", shift(S, d)) for d in range(1, S)]
        over_rhs = []
        for s in range(S):
            piece = pick(over_col, (q - p - s) % S)
            over_rhs.append(piece if s == 0 else lax.ppermute(piece, "rhs", shift(S, s)))
        ordered = [pick(over_rhs, (p - x) % S) for x in range(S)]
        halves.append(jnp.stack(ordered, axis=1).reshape(HALF, m))

    table = jnp.asarray(pack_table())
    mine = lax.dynamic_index_in_dim(table, t, 0, keepdims=False)
    meta = jnp.concatenate([t[None], mine.reshape(-1), p[None]]).astype(jnp.int32)
    vmem = pl.BlockSpec(memory_space=pltpu.VMEM)
    smem = pl.BlockSpec(memory_space=pltpu.SMEM)
    sends = pl.pallas_call(
        old_send_kernel,
        in_specs=[vmem, vmem],
        out_specs=vmem,
        out_shape=jax.ShapeDtypeStruct((NB, S, 8, 128), F32),
        compiler_params=pltpu.CompilerParams(vmem_limit_bytes=8 * 2**20),
        name="old_send",
    )(guess[0], right)
    arrived = lax.all_to_all(sends.reshape(NB * S, 8, 128), ("row", "col"), 0, 0, tiled=True)
    arrived = arrived.reshape(NB, S, 8, 128)
    own_old = pl.pallas_call(
        old_sum_kernel,
        in_specs=[smem, smem, vmem],
        out_specs=vmem,
        out_shape=jax.ShapeDtypeStruct((NB, 8, 128), BF),
        compiler_params=pltpu.CompilerParams(vmem_limit_bytes=8 * 2**20),
        name="old_sum",
    )(meta, ranks, arrived)
    packed_old = [own_old] + [lax.ppermute(own_old, "rhs", shift(S, s)) for s in range(1, S)]

    x0, h0 = pl.pallas_call(
        first_kernel,
        in_specs=[vmem] * 3,
        out_specs=[vmem] * 2,
        out_shape=[
            jax.ShapeDtypeStruct((HALF, m), BF),
            jax.ShapeDtypeStruct((4, HALF, 128), F32),
        ],
        compiler_params=pltpu.CompilerParams(vmem_limit_bytes=20 * 2**20),
        name="first",
    )(halves[0], inverse[0], right)
    x1, packed, old = pl.pallas_call(
        second_kernel,
        in_specs=[smem] + [vmem] * 8,
        out_specs=[vmem] * 3,
        out_shape=[
            jax.ShapeDtypeStruct((HALF, m), BF),
            jax.ShapeDtypeStruct((16, 32, 128), BF),
            jax.ShapeDtypeStruct((R, NB * K), BF),
        ],
        scratch_shapes=[pltpu.VMEM((4, NB * K, 128), F32)],
        compiler_params=pltpu.CompilerParams(vmem_limit_bytes=22 * 2**20),
        name="second",
    )(meta, halves[1], inverse[0], right, *packed_old, h0)

    summed = lax.all_to_all(packed, ("col", "rhs"), 0, 0, tiled=True)
    summed = summed.astype(F32).sum(axis=0).astype(BF)
    shared = lax.all_to_all(
        jnp.broadcast_to(summed[None], (128, 32, 128)), ("row", "col", "rhs"), 0, 0, tiled=True
    ).reshape(NB, 16, 32, 128)

    partial_solution = pl.pallas_call(
        chain_kernel,
        in_specs=[smem, smem, vmem, vmem, vmem, vmem],
        out_specs=vmem,
        out_shape=jax.ShapeDtypeStruct((R, m), F32),
        scratch_shapes=[pltpu.VMEM((NB, R, NB * K), BF)],
        compiler_params=pltpu.CompilerParams(vmem_limit_bytes=16 * 2**20),
        name="sweep",
    )(meta, ranks, shared, old, x0, x1)

    result = lax.dynamic_slice(partial_solution, (16 * p, 0), (16, m))
    for s in range(1, S):
        send = lax.dynamic_slice(partial_solution, (16 * ((p + s) % S), 0), (16, m)).astype(BF)
        result = result + lax.ppermute(send, "rhs", shift(S, s)).astype(F32)
    return result[None]


def solution(mesh):
    in_specs = (
        P("row", "rhs", "col"),
        P("row", "rhs", "col"),
        P("row", "rhs", "col"),
        P("row", None, None, "col"),
        P("row", None, None, "col"),
        P(),
    )
    out_specs = P("row", "rhs", "col")
    return jax.shard_map(program, mesh=mesh, in_specs=in_specs, out_specs=out_specs, check_vma=False)
```

```python
import numpy as np

import jax
import jax.numpy as jnp
from jax import lax
from jax.experimental import pallas as pl
from jax.experimental.pallas import tpu as pltpu
from jax.sharding import PartitionSpec as P


NB, K, R, S = 8, 64, 64, 4
PARTS = 2
HALF = NB * K // PARTS
BF = jnp.bfloat16
F32 = jnp.float32


def pack_table():
    table = np.zeros((NB, 2, 16), np.int32)
    for t in range(NB):
        pairs = [(j, i) for j in range(t + 1) for i in range(t + 1, NB)]
        for s, (j, i) in enumerate(pairs):
            table[t, :, s] = (j, i)
    return table


def shift(axis_size, by):
    return [(i, (i + by) % axis_size) for i in range(axis_size)]


def pick(arrays, index):
    out = arrays[-1]
    for n in range(len(arrays) - 2, -1, -1):
        out = jnp.where(index == n, arrays[n], out)
    return out


def nt_dot(a, b):
    return lax.dot_general(a, b, (((1,), (1,)), ((), ())), preferred_element_type=F32)


def old_send_kernel(guess_ref, r_ref, out_ref):
    product = nt_dot(guess_ref[...].astype(BF), r_ref[...])
    left = lax.broadcasted_iota(jnp.int32, (8, 128), 1) < 64
    for m in range(NB // 2):
        upper = product[:8, m * 128 : (m + 1) * 128]
        lower = product[8:, m * 128 : (m + 1) * 128]
        even = jnp.where(left, upper, pltpu.roll(lower, 64, 1))
        odd = jnp.where(left, pltpu.roll(upper, 64, 1), lower)
        for d in range(S):
            out_ref[2 * m, d] = even
            out_ref[2 * m + 1, d] = odd


def old_sum_kernel(meta, ranks, in_ref, out_ref):
    t = meta[0]
    column = lax.broadcasted_iota(jnp.int32, (8, 128), 1) % K
    for j in range(NB):
        total = (in_ref[j, 0] + in_ref[j, 1]) + (in_ref[j, 2] + in_ref[j, 3])
        rank = jnp.where(t < j, ranks[t, j], 0)
        out_ref[j] = jnp.where(column < rank, total, 0.0).astype(BF)


def unpack_old(meta, packed, old_ref):
    left = lax.broadcasted_iota(jnp.int32, (8, 128), 1) < 64
    for s, packed_ref in enumerate(packed):
        source = (meta[33] + (S - s)) % S
        rows = pl.ds(pl.multiple_of(source * 16, 16), 16)
        for m in range(NB // 2):
            even = packed_ref[2 * m].astype(F32)
            odd = packed_ref[2 * m + 1].astype(F32)
            upper = jnp.where(left, even, pltpu.roll(odd, 64, 1))
            lower = jnp.where(left, pltpu.roll(even, 64, 1), odd)
            both = jnp.concatenate([upper, lower], axis=0).astype(BF)
            old_ref[rows, m * 128 : (m + 1) * 128] = both


def first_kernel(a_ref, inv_ref, r_ref, x_ref, h_ref):
    x_ref[...] = jnp.dot(a_ref[...], inv_ref[...], preferred_element_type=F32).astype(BF)
    part = nt_dot(x_ref[...], r_ref[...])
    for m in range(4):
        h_ref[m] = part[:, m * 128 : (m + 1) * 128]


def second_kernel(
    meta, a_ref, inv_ref, r_ref, o0, o1, o2, o3, h0_ref, x_ref, pack_ref, old_ref, h_s
):
    unpack_old(meta, (o0, o1, o2, o3), old_ref)
    for m in range(4):
        h_s[m, :HALF] = h0_ref[m]
    x_ref[...] = jnp.dot(a_ref[...], inv_ref[...], preferred_element_type=F32).astype(BF)
    part = nt_dot(x_ref[...], r_ref[...])
    for m in range(4):
        h_s[m, HALF:] = part[:, m * 128 : (m + 1) * 128]
    own = pl.ds(pl.multiple_of(meta[0] * K, K), K)
    for m in range(4):
        fold = jnp.dot(old_ref[...], h_s[m].astype(BF), preferred_element_type=F32)
        h_s[m, own, :] = h_s[m, own, :] - fold
    lane = lax.broadcasted_iota(jnp.int32, (32, 128), 1)
    for s in range(16):
        j = meta[1 + s]
        i = meta[17 + s]
        block = h_s[i // 2, pl.ds(pl.multiple_of(j * K, K), K), :]
        swapped = pltpu.roll(block, 64, 1)
        odd = (i % 2) == 1
        even_lanes = jnp.where(odd, swapped, block)
        odd_lanes = jnp.where(odd, block, swapped)
        pack_ref[s] = jnp.where(lane < 64, even_lanes[:32], odd_lanes[32:]).astype(BF)


def chain_kernel(meta, ranks, hg_ref, old_ref, x0_ref, x1_ref, out_ref, c_s):
    def block(t, s):
        packed = hg_ref[t, s]
        return jnp.concatenate([packed[:, :64], packed[:, 64:]], axis=0)

    coef = {}
    lane = lax.broadcasted_iota(jnp.int32, (R, K), 1)
    c_s[0] = jnp.zeros((R, NB * K), BF)
    for t in range(NB):
        count = NB - 1 - t
        if t > 0:
            incoming = [coef[j, t] for j in range(t)]
            filler = [jnp.zeros((R, K), BF)] * (NB - t)
            c_s[t] = jnp.concatenate(incoming + filler, axis=1)
        if count == 0:
            break
        y = jnp.concatenate([block(t, t * count + b) for b in range(count)], axis=1).astype(F32)
        if t > 0:
            g = jnp.concatenate(
                [
                    jnp.concatenate([block(t, a * count + b) for b in range(count)], axis=1)
                    for a in range(t)
                ],
                axis=0,
            )
            y = y - jnp.dot(jnp.concatenate(incoming, axis=1), g, preferred_element_type=F32)
        for b in range(count):
            i = t + 1 + b
            piece = y[:, b * K : (b + 1) * K]
            coef[t, i] = jnp.where(lane < ranks[i, t], piece, 0.0).astype(BF)
    mine = meta[0]
    total = c_s[mine] + old_ref[...]
    own = pl.ds(pl.multiple_of((mine % 4) * K, K), K)
    own_rows = jnp.where(mine < 4, x0_ref[own, :], x1_ref[own, :])
    sums = jnp.dot(total[:, :HALF], x0_ref[...], preferred_element_type=F32)
    sums = sums + jnp.dot(total[:, HALF:], x1_ref[...], preferred_element_type=F32)
    out_ref[...] = own_rows.astype(F32) - sums


def program(right_side, guess, inverse, left_factor, right_factor, ranks):
    t = lax.axis_index("row")
    q = lax.axis_index("col")
    p = lax.axis_index("rhs")
    left = left_factor[0]
    right = right_factor[0].reshape(NB * K, -1)
    m = left.shape[2]

    per = NB // PARTS
    own_rows = right_side[0].astype(BF)[None]
    parts = []
    for n in range(PARTS):
        part = lax.dynamic_slice(left, (n * per, 16 * p, 0), (per, 16, m))
        own_block = lax.broadcasted_iota(jnp.int32, (per, 1, 1), 0) + n * per == t
        parts.append(jnp.where(own_block, own_rows, part))
    parts = lax.optimization_barrier(tuple(parts))
    halves = []
    for n in range(PARTS):
        part = parts[n]
        over_col = [part] + [lax.ppermute(part, "col", shift(S, d)) for d in range(1, S)]
        over_rhs = []
        pieces = tuple(pick(over_col, (q - p - s) % S) for s in range(S))
        pieces = lax.optimization_barrier(pieces)
        for s in range(S):
            piece = pieces[s]
            over_rhs.append(piece if s == 0 else lax.ppermute(piece, "rhs", shift(S, s)))
        ordered = [pick(over_rhs, (p - x) % S) for x in range(S)]
        halves.append(jnp.stack(ordered, axis=1).reshape(HALF, m))

    table = jnp.asarray(pack_table())
    mine = lax.dynamic_index_in_dim(table, t, 0, keepdims=False)
    meta = jnp.concatenate([t[None], mine.reshape(-1), p[None]]).astype(jnp.int32)
    vmem = pl.BlockSpec(memory_space=pltpu.VMEM)
    smem = pl.BlockSpec(memory_space=pltpu.SMEM)
    sends = pl.pallas_call(
        old_send_kernel,
        in_specs=[vmem, vmem],
        out_specs=vmem,
        out_shape=jax.ShapeDtypeStruct((NB, S, 8, 128), F32),
        compiler_params=pltpu.CompilerParams(vmem_limit_bytes=8 * 2**20),
        name="old_send",
    )(guess[0], right)
    arrived = lax.all_to_all(sends.reshape(NB * S, 8, 128), ("row", "col"), 0, 0, tiled=True)
    arrived = arrived.reshape(NB, S, 8, 128)
    own_old = pl.pallas_call(
        old_sum_kernel,
        in_specs=[smem, smem, vmem],
        out_specs=vmem,
        out_shape=jax.ShapeDtypeStruct((NB, 8, 128), BF),
        compiler_params=pltpu.CompilerParams(vmem_limit_bytes=8 * 2**20),
        name="old_sum",
    )(meta, ranks, arrived)
    packed_old = [own_old] + [lax.ppermute(own_old, "rhs", shift(S, s)) for s in range(1, S)]

    x0, h0 = pl.pallas_call(
        first_kernel,
        in_specs=[vmem] * 3,
        out_specs=[vmem] * 2,
        out_shape=[
            jax.ShapeDtypeStruct((HALF, m), BF),
            jax.ShapeDtypeStruct((4, HALF, 128), F32),
        ],
        compiler_params=pltpu.CompilerParams(vmem_limit_bytes=34 * 2**20),
        name="first",
    )(halves[0], inverse[0], right)
    x1, packed, old = pl.pallas_call(
        second_kernel,
        in_specs=[smem] + [vmem] * 8,
        out_specs=[vmem] * 3,
        out_shape=[
            jax.ShapeDtypeStruct((HALF, m), BF),
            jax.ShapeDtypeStruct((16, 32, 128), BF),
            jax.ShapeDtypeStruct((R, NB * K), BF),
        ],
        scratch_shapes=[pltpu.VMEM((4, NB * K, 128), F32)],
        compiler_params=pltpu.CompilerParams(vmem_limit_bytes=20 * 2**20),
        name="second",
    )(meta, halves[1], inverse[0], right, *packed_old, h0)

    summed = lax.all_to_all(packed, ("col", "rhs"), 0, 0, tiled=True)
    summed = summed.astype(F32).sum(axis=0).astype(BF)
    shared = lax.all_to_all(
        jnp.broadcast_to(summed[None], (128, 32, 128)), ("row", "col", "rhs"), 0, 0, tiled=True
    ).reshape(NB, 16, 32, 128)

    partial_solution = pl.pallas_call(
        chain_kernel,
        in_specs=[smem, smem, vmem, vmem, vmem, vmem],
        out_specs=vmem,
        out_shape=jax.ShapeDtypeStruct((R, m), F32),
        scratch_shapes=[pltpu.VMEM((NB, R, NB * K), BF)],
        compiler_params=pltpu.CompilerParams(vmem_limit_bytes=16 * 2**20),
        name="sweep",
    )(meta, ranks, shared, old, x0, x1)

    result = lax.dynamic_slice(partial_solution, (16 * p, 0), (16, m))
    for s in range(1, S):
        send = lax.dynamic_slice(partial_solution, (16 * ((p + s) % S), 0), (16, m)).astype(BF)
        result = result + lax.ppermute(send, "rhs", shift(S, s)).astype(F32)
    return result[None]


def solution(mesh):
    in_specs = (
        P("row", "rhs", "col"),
        P("row", "rhs", "col"),
        P("row", "rhs", "col"),
        P("row", None, None, "col"),
        P("row", None, None, "col"),
        P(),
    )
    out_specs = P("row", "rhs", "col")
    return jax.shard_map(program, mesh=mesh, in_specs=in_specs, out_specs=out_specs, check_vma=False)
```

```python
import numpy as np

import jax
import jax.numpy as jnp
from jax import lax
from jax.experimental import pallas as pl
from jax.experimental.pallas import tpu as pltpu
from jax.sharding import PartitionSpec as P


NB, K, R, S = 8, 64, 64, 4
PARTS = 2
HALF = NB * K // PARTS
BF = jnp.bfloat16
F32 = jnp.float32


def pack_table():
    table = np.zeros((NB, 2, 16), np.int32)
    for t in range(NB):
        pairs = [(j, i) for j in range(t + 1) for i in range(t + 1, NB)]
        for s, (j, i) in enumerate(pairs):
            table[t, :, s] = (j, i)
    return table


def shift(axis_size, by):
    return [(i, (i + by) % axis_size) for i in range(axis_size)]


def pick(arrays, index):
    out = arrays[-1]
    for n in range(len(arrays) - 2, -1, -1):
        out = jnp.where(index == n, arrays[n], out)
    return out


def nt_dot(a, b):
    return lax.dot_general(a, b, (((1,), (1,)), ((), ())), preferred_element_type=F32)


def old_send_kernel(guess_ref, r_ref, out_ref):
    product = nt_dot(guess_ref[...].astype(BF), r_ref[...])
    left = lax.broadcasted_iota(jnp.int32, (8, 128), 1) < 64
    for m in range(NB // 2):
        upper = product[:8, m * 128 : (m + 1) * 128]
        lower = product[8:, m * 128 : (m + 1) * 128]
        even = jnp.where(left, upper, pltpu.roll(lower, 64, 1))
        odd = jnp.where(left, pltpu.roll(upper, 64, 1), lower)
        for d in range(S):
            out_ref[2 * m, d] = even
            out_ref[2 * m + 1, d] = odd


def old_sum_kernel(meta, ranks, in_ref, out_ref):
    t = meta[0]
    column = lax.broadcasted_iota(jnp.int32, (8, 128), 1) % K
    for j in range(NB):
        total = (in_ref[j, 0] + in_ref[j, 1]) + (in_ref[j, 2] + in_ref[j, 3])
        rank = jnp.where(t < j, ranks[t, j], 0)
        out_ref[j] = jnp.where(column < rank, total, 0.0).astype(BF)


def unpack_old(meta, packed, old_ref):
    left = lax.broadcasted_iota(jnp.int32, (8, 128), 1) < 64
    for s, packed_ref in enumerate(packed):
        source = (meta[33] + (S - s)) % S
        rows = pl.ds(pl.multiple_of(source * 16, 16), 16)
        for m in range(NB // 2):
            even = packed_ref[2 * m].astype(F32)
            odd = packed_ref[2 * m + 1].astype(F32)
            upper = jnp.where(left, even, pltpu.roll(odd, 64, 1))
            lower = jnp.where(left, pltpu.roll(even, 64, 1), odd)
            both = jnp.concatenate([upper, lower], axis=0).astype(BF)
            old_ref[rows, m * 128 : (m + 1) * 128] = both


def first_kernel(a_ref, inv_ref, x_ref):
    x_ref[...] = jnp.dot(a_ref[...], inv_ref[...], preferred_element_type=F32).astype(BF)


def second_kernel(
    meta, a_ref, inv_ref, r_ref, o0, o1, o2, o3, x0_ref, x_ref, pack_ref, old_ref, h_s
):
    unpack_old(meta, (o0, o1, o2, o3), old_ref)
    part = nt_dot(x0_ref[...], r_ref[...])
    for m in range(4):
        h_s[m, :HALF] = part[:, m * 128 : (m + 1) * 128]
    x_ref[...] = jnp.dot(a_ref[...], inv_ref[...], preferred_element_type=F32).astype(BF)
    part = nt_dot(x_ref[...], r_ref[...])
    for m in range(4):
        h_s[m, HALF:] = part[:, m * 128 : (m + 1) * 128]
    own = pl.ds(pl.multiple_of(meta[0] * K, K), K)
    for m in range(4):
        fold = jnp.dot(old_ref[...], h_s[m].astype(BF), preferred_element_type=F32)
        h_s[m, own, :] = h_s[m, own, :] - fold
    lane = lax.broadcasted_iota(jnp.int32, (32, 128), 1)
    for s in range(16):
        j = meta[1 + s]
        i = meta[17 + s]
        block = h_s[i // 2, pl.ds(pl.multiple_of(j * K, K), K), :]
        swapped = pltpu.roll(block, 64, 1)
        odd = (i % 2) == 1
        even_lanes = jnp.where(odd, swapped, block)
        odd_lanes = jnp.where(odd, block, swapped)
        pack_ref[s] = jnp.where(lane < 64, even_lanes[:32], odd_lanes[32:]).astype(BF)


def chain_kernel(meta, ranks, hg_ref, old_ref, x0_ref, x1_ref, out_ref, c_s):
    def block(t, s):
        packed = hg_ref[t, s]
        return jnp.concatenate([packed[:, :64], packed[:, 64:]], axis=0)

    coef = {}
    lane = lax.broadcasted_iota(jnp.int32, (R, K), 1)
    c_s[0] = jnp.zeros((R, NB * K), BF)
    for t in range(NB):
        count = NB - 1 - t
        if t > 0:
            incoming = [coef[j, t] for j in range(t)]
            filler = [jnp.zeros((R, K), BF)] * (NB - t)
            c_s[t] = jnp.concatenate(incoming + filler, axis=1)
        if count == 0:
            break
        y = jnp.concatenate([block(t, t * count + b) for b in range(count)], axis=1).astype(F32)
        if t > 0:
            g = jnp.concatenate(
                [
                    jnp.concatenate([block(t, a * count + b) for b in range(count)], axis=1)
                    for a in range(t)
                ],
                axis=0,
            )
            y = y - jnp.dot(jnp.concatenate(incoming, axis=1), g, preferred_element_type=F32)
        for b in range(count):
            i = t + 1 + b
            piece = y[:, b * K : (b + 1) * K]
            coef[t, i] = jnp.where(lane < ranks[i, t], piece, 0.0).astype(BF)
    mine = meta[0]
    total = c_s[mine] + old_ref[...]
    own = pl.ds(pl.multiple_of((mine % 4) * K, K), K)
    own_rows = jnp.where(mine < 4, x0_ref[own, :], x1_ref[own, :])
    sums = jnp.dot(total[:, :HALF], x0_ref[...], preferred_element_type=F32)
    sums = sums + jnp.dot(total[:, HALF:], x1_ref[...], preferred_element_type=F32)
    out_ref[...] = own_rows.astype(F32) - sums


def program(right_side, guess, inverse, left_factor, right_factor, ranks):
    t = lax.axis_index("row")
    q = lax.axis_index("col")
    p = lax.axis_index("rhs")
    left = left_factor[0]
    right = right_factor[0].reshape(NB * K, -1)
    m = left.shape[2]

    per = NB // PARTS
    own_rows = right_side[0].astype(BF)[None]
    parts = []
    for n in range(PARTS):
        part = lax.dynamic_slice(left, (n * per, 16 * p, 0), (per, 16, m))
        own_block = lax.broadcasted_iota(jnp.int32, (per, 1, 1), 0) + n * per == t
        parts.append(jnp.where(own_block, own_rows, part))
    parts = lax.optimization_barrier(tuple(parts))
    halves = []
    for n in range(PARTS):
        part = parts[n]
        over_col = [part] + [lax.ppermute(part, "col", shift(S, d)) for d in range(1, S)]
        over_rhs = []
        pieces = tuple(pick(over_col, (q - p - s) % S) for s in range(S))
        pieces = lax.optimization_barrier(pieces)
        for s in range(S):
            piece = pieces[s]
            over_rhs.append(piece if s == 0 else lax.ppermute(piece, "rhs", shift(S, s)))
        ordered = [pick(over_rhs, (p - x) % S) for x in range(S)]
        halves.append(jnp.stack(ordered, axis=1).reshape(HALF, m))

    table = jnp.asarray(pack_table())
    mine = lax.dynamic_index_in_dim(table, t, 0, keepdims=False)
    meta = jnp.concatenate([t[None], mine.reshape(-1), p[None]]).astype(jnp.int32)
    vmem = pl.BlockSpec(memory_space=pltpu.VMEM)
    smem = pl.BlockSpec(memory_space=pltpu.SMEM)
    sends = pl.pallas_call(
        old_send_kernel,
        in_specs=[vmem, vmem],
        out_specs=vmem,
        out_shape=jax.ShapeDtypeStruct((NB, S, 8, 128), F32),
        compiler_params=pltpu.CompilerParams(vmem_limit_bytes=8 * 2**20),
        name="old_send",
    )(guess[0], right)
    arrived = lax.all_to_all(sends.reshape(NB * S, 8, 128), ("row", "col"), 0, 0, tiled=True)
    arrived = arrived.reshape(NB, S, 8, 128)
    own_old = pl.pallas_call(
        old_sum_kernel,
        in_specs=[smem, smem, vmem],
        out_specs=vmem,
        out_shape=jax.ShapeDtypeStruct((NB, 8, 128), BF),
        compiler_params=pltpu.CompilerParams(vmem_limit_bytes=8 * 2**20),
        name="old_sum",
    )(meta, ranks, arrived)
    packed_old = [own_old] + [lax.ppermute(own_old, "rhs", shift(S, s)) for s in range(1, S)]

    x0 = pl.pallas_call(
        first_kernel,
        in_specs=[vmem] * 2,
        out_specs=vmem,
        out_shape=jax.ShapeDtypeStruct((HALF, m), BF),
        compiler_params=pltpu.CompilerParams(vmem_limit_bytes=34 * 2**20),
        name="first",
    )(halves[0], inverse[0])
    x1, packed, old = pl.pallas_call(
        second_kernel,
        in_specs=[smem] + [vmem] * 8,
        out_specs=[vmem] * 3,
        out_shape=[
            jax.ShapeDtypeStruct((HALF, m), BF),
            jax.ShapeDtypeStruct((16, 32, 128), BF),
            jax.ShapeDtypeStruct((R, NB * K), BF),
        ],
        scratch_shapes=[pltpu.VMEM((4, NB * K, 128), F32)],
        compiler_params=pltpu.CompilerParams(vmem_limit_bytes=20 * 2**20),
        name="second",
    )(meta, halves[1], inverse[0], right, *packed_old, x0)

    summed = lax.all_to_all(packed, ("col", "rhs"), 0, 0, tiled=True)
    summed = summed.astype(F32).sum(axis=0).astype(BF)
    shared = lax.all_to_all(
        jnp.broadcast_to(summed[None], (128, 32, 128)), ("row", "col", "rhs"), 0, 0, tiled=True
    ).reshape(NB, 16, 32, 128)

    partial_solution = pl.pallas_call(
        chain_kernel,
        in_specs=[smem, smem, vmem, vmem, vmem, vmem],
        out_specs=vmem,
        out_shape=jax.ShapeDtypeStruct((R, m), F32),
        scratch_shapes=[pltpu.VMEM((NB, R, NB * K), BF)],
        compiler_params=pltpu.CompilerParams(vmem_limit_bytes=16 * 2**20),
        name="sweep",
    )(meta, ranks, shared, old, x0, x1)

    result = lax.dynamic_slice(partial_solution, (16 * p, 0), (16, m))
    for s in range(1, S):
        send = lax.dynamic_slice(partial_solution, (16 * ((p + s) % S), 0), (16, m)).astype(BF)
        result = result + lax.ppermute(send, "rhs", shift(S, s)).astype(F32)
    return result[None]


def solution(mesh):
    in_specs = (
        P("row", "rhs", "col"),
        P("row", "rhs", "col"),
        P("row", "rhs", "col"),
        P("row", None, None, "col"),
        P("row", None, None, "col"),
        P(),
    )
    out_specs = P("row", "rhs", "col")
    return jax.shard_map(program, mesh=mesh, in_specs=in_specs, out_specs=out_specs, check_vma=False)
```
